32 devices in a mesh: gx: 4 (over y, core), gy: 8 (over z, x).
Axes of the slice: x: 2, y: 2, z: 4, core: 2. Of those that a mesh axis runs over, the one named last changes fastest.
Arguments:
- emission: float32 [512, 8, 128], P(('gx', 'gy')), may hold values from 0.05 to 1
- reflectance: float32 [512, 8, 128], P(('gx', 'gy')), may hold values from 0.5 to 0.98
- form_factors: float32 [8192, 128, 128], P(('gx', 'gy')), as said below
- link_source: int32 [8192], P(('gx', 'gy')), may hold values from 0 to 511, as said below
- link_target: int32 [8192], P(('gx', 'gy')), may hold values from 0 to 511, as said below
- link_length: int32 [8192], P(('gx', 'gy')), may hold values from 32 to 128
- block_count: int32 [32], P(('gx', 'gy')), may hold values from 32 to 256, as said below
Outputs:
- solution: float32 [512, 8, 128], P(('gx', 'gy'))
- residual: float32 [512, 8, 128], P(('gx', 'gy'))
The draws below stay inside these ranges and needn't reach their ends.
Inputs may be any that keep to these rules, and one draw needn't show every extreme that they name: `form_factors`: entries are nonnegative. `link_source`: block k's source is any cluster; among the blocks held by one device, all blocks whose sources lie on one same device name the same source cluster. `link_target`: block k's target is one of the clusters of the device holding it, clusters (k // 256) * 16 to (k // 256) * 16 + 15. `block_count`: some device has all 256 slots live.
All inputs are finite; a program needn't handle non-finite values.
Results may differ from the reference program's by a relative error of at most 0.0011.
Values sent between devices are 32-bit elements; how exact they have to be, the bound alone decides.
A program may use at most 64 MiB of HBM per device.

```python
import math
import jax
import jax.numpy as jnp
from jax import lax

CL = 128
BANDS = 8
CPD = 16
BLK_DEV = 256
ITERS = 3
NCL = 512
NBLK = 8192
DEVICES = 32


def count_table(key):
    roll_draw = jax.random.randint(jax.random.fold_in(key, 11), (DEVICES,), 0, 8)
    least_count = max(1, BLK_DEV // 8)
    counts = least_count + (BLK_DEV - least_count) * (roll_draw * roll_draw * roll_draw) // 343
    full_dev = jax.random.randint(jax.random.fold_in(key, 12), (), 0, DEVICES)
    return jnp.where(jnp.arange(DEVICES, dtype=jnp.int32) == full_dev, BLK_DEV, counts).astype(jnp.int32)


def draw_block_count(key, part):
    return count_table(key)


def draw_link_source(key, part):
    block_ids = jnp.arange(NBLK, dtype=jnp.int32)
    holder = block_ids // BLK_DEV
    slot_index = block_ids % BLK_DEV
    random_peer = jax.random.randint(jax.random.fold_in(key, 21), (NBLK,), 0, DEVICES)
    far_peer = (holder + DEVICES // 2) % DEVICES
    next_peer = (holder + 1) % DEVICES
    peer_dev = jnp.where(slot_index == 0, far_peer, jnp.where(slot_index == 1, next_peer, random_peer))
    stride_draw = jax.random.randint(jax.random.fold_in(key, 22), (2,), 0, CPD)
    slot_pick = 1 + (holder + peer_dev * (2 * stride_draw[0] + 1) + stride_draw[1]) % (CPD - 1)
    return (peer_dev * CPD + slot_pick).astype(jnp.int32)


def draw_link_target(key, part):
    holder = jnp.arange(NBLK, dtype=jnp.int32) // BLK_DEV
    local_pick = jax.random.randint(jax.random.fold_in(key, 23), (NBLK,), 0, CPD)
    return (holder * CPD + local_pick).astype(jnp.int32)


def draw_form_factors(key, part):
    counts = count_table(key)
    holder = jnp.arange(NBLK, dtype=jnp.int32) // BLK_DEV
    block_scale = 1.4 * CPD / (counts[holder].astype(jnp.float32) * CL)
    uniform_draw = jax.random.uniform(jax.random.fold_in(key, 31), (NBLK, CL, CL), jnp.float32)
    return uniform_draw * block_scale[:, None, None]


def place_ends(array, rng, least, high):
    spot = [jax.random.randint(jax.random.fold_in(rng, axis), (), 0, length) for axis, length in enumerate(array.shape)]
    longest = array.shape.index(max(array.shape))
    next_to = spot[:longest] + [(spot[longest] + 1) % array.shape[longest]] + spot[longest + 1:]
    return array.at[tuple(spot)].set(least).at[tuple(next_to)].set(high)


def level_of(own_key, extent, shards, smallest, top_value):
    gain, own = 1.0, jax.random.fold_in(own_key, 6)
    for position, shards_of in shards:
        heights = jnp.exp(jax.random.uniform(jax.random.fold_in(own, position), (shards_of,), jnp.float32, smallest / len(shards), top_value / len(shards)))
        gain = gain * jnp.repeat(heights, extent[position] // shards_of).reshape([-1 if axis == position else 1 for axis in range(len(extent))])
    return gain


def setup_inputs(seed: int = 0) -> dict:
    key_of = jax.random.split(jax.random.key(seed), 8)
    emission = jnp.clip(jnp.exp(math.log(1.0) - 2.9957323 * jax.random.uniform(key_of[0], (NCL, BANDS, CL), jnp.float32) ** level_of(key_of[0], (NCL, BANDS, CL), ((0, 32),), -0.2, 0.2)), 0.05, 1.0)
    reflectance = jnp.clip(jnp.exp(math.log(0.98) - 0.6729445 * jax.random.uniform(key_of[1], (NCL, BANDS, CL), jnp.float32) ** level_of(key_of[1], (NCL, BANDS, CL), ((0, 32),), -0.2, 0.2)), 0.5, 0.98)
    form_factors = draw_form_factors(jax.random.fold_in(key_of[7], 71), 0)
    link_source = draw_link_source(jax.random.fold_in(key_of[7], 71), 0)
    link_target = draw_link_target(jax.random.fold_in(key_of[7], 71), 0)
    link_length = place_ends(jax.random.randint(key_of[5], (NBLK,), CL // 4, CL + 1), jax.random.fold_in(key_of[5], 1), CL // 4, CL).astype(jnp.int32)
    block_count = draw_block_count(jax.random.fold_in(key_of[7], 71), 0)
    return dict(emission=emission, reflectance=reflectance, form_factors=form_factors, link_source=link_source, link_target=link_target, link_length=link_length, block_count=block_count)


def apply_operator(radiance, reflectance, form_factors, link_source, link_target, link_length, block_count):
    column_ids = jnp.arange(CL, dtype=jnp.int32)
    slot_ids = jnp.arange(BLK_DEV, dtype=jnp.int32)
    float_type = radiance.dtype

    def per_device(total, inputs):
        factors, source_ids, target_ids, lengths, live_count = inputs
        live_block = slot_ids < live_count
        column_mask = ((column_ids[None, :] < lengths[:, None]) & live_block[:, None]).astype(float_type)
        source_vals = radiance[source_ids] * column_mask[:, None, :]
        partial_sum = jnp.einsum("kij,kbj->kbi", factors, source_vals, precision=lax.Precision.HIGHEST)
        total = total + jax.ops.segment_sum(partial_sum, target_ids, num_segments=NCL)
        return total, None

    inputs = (form_factors.reshape(DEVICES, BLK_DEV, CL, CL),
              link_source.reshape(DEVICES, BLK_DEV),
              link_target.reshape(DEVICES, BLK_DEV),
              link_length.reshape(DEVICES, BLK_DEV),
              block_count)
    gathered, _ = lax.scan(per_device, jnp.zeros_like(radiance), inputs)
    return radiance - reflectance * gathered


def reference(emission, reflectance, form_factors, link_source, link_target, link_length, block_count):
    def operate(radiance):
        return apply_operator(radiance, reflectance, form_factors, link_source, link_target, link_length, block_count)

    float_type = emission.dtype
    solution = jnp.zeros_like(emission)
    residual = emission
    shadow = emission
    direction = jnp.zeros_like(emission)
    applied = jnp.zeros_like(emission)
    rho_old = jnp.ones((), float_type)
    alpha_coef = jnp.ones((), float_type)
    omega_coef = jnp.ones((), float_type)
    for iteration in range(ITERS):
        rho_new = jnp.sum(shadow * residual)
        beta_coef = (rho_new / rho_old) * (alpha_coef / omega_coef)
        direction = residual + beta_coef * (direction - omega_coef * applied)
        applied = operate(direction)
        alpha_coef = rho_new / jnp.sum(shadow * applied)
        middle = residual - alpha_coef * applied
        bounce = operate(middle)
        omega_coef = jnp.sum(bounce * middle) / jnp.sum(bounce * bounce)
        solution = solution + alpha_coef * direction + omega_coef * middle
        residual = middle - omega_coef * bounce
        rho_old = rho_new
    return solution, residual
```

```python
import jax
import jax.numpy as jnp
from jax import lax
from jax.sharding import PartitionSpec as P
from jax.experimental import pallas as pl
from jax.experimental.pallas import tpu as pltpu

ITERS = 3
PHASES = 2 * ITERS + 1
CHUNK = 16
SLOTS = 4
UNROLL = 128
EARLY = 6


def divide(x, by):
    if by & (by - 1) == 0:
        return lax.shift_right_logical(x, by.bit_length() - 1), lax.bitwise_and(x, by - 1)
    return lax.div(x, by), lax.rem(x, by)


def partners(index, size):
    if size & (size - 1):
        return [lax.rem(index + a, size) for a in range(size)]
    flips = [(1 << b) - 2 * (1 << b) * lax.rem(lax.div(index, 1 << b), 2) for b in range(size.bit_length() - 1)]
    out = []
    for a in range(size):
        p = index
        for b, flip in enumerate(flips):
            if a >> b & 1:
                p = p + flip
        out.append(p)
    return out


def kernel(len_h, count_h, source_h, target_h, em_h, refl_h, ff, sol, res,
           w, stage, runs, vt, outb, inb, dout, din, em, refl, image, direction, total, rs, ds,
           wout, win, want_s, ints_v, ints_s, reals_v, reals_s, source_v, target_v, len_s, count_s,
           stage_sem, send_sem, recv_sem, ssend_sem, srecv_sem, wsend_sem, wrecv_sem, small_sem):
    nx, ny = lax.axis_size("gx"), lax.axis_size("gy")
    n = nx * ny
    gx, gy = lax.axis_index("gx"), lax.axis_index("gy")
    me = gx * ny + gy
    clusters = em.shape[0]
    blocks, cl = ff.shape[0], ff.shape[2]
    chunks = blocks // CHUNK
    i32, f32, bf16 = jnp.int32, jnp.float32, jnp.bfloat16

    pxs, pys = partners(gx, nx), partners(gy, ny)
    order = sorted(
        ((a, b) for a in range(nx) for b in range(ny) if a or b),
        key=lambda q: (-bin(q[0] >> 1).count("1") - (q[1] & 1), -(q[0] & 1), -q[1]))

    def each_peer(act):
        for a, b in order:
            act(pxs[a], pys[b])

    barrier = pltpu.get_barrier_semaphore()
    each_peer(lambda px, py: pl.semaphore_signal(
        barrier, inc=1, device_id=(px, py), device_id_type=pl.DeviceIdType.MESH))

    def fetch(c, slot):
        return pltpu.make_async_copy(ff.at[pl.ds(c * CHUNK, CHUNK)], stage.at[slot], stage_sem.at[slot])

    inputs = [pltpu.make_async_copy(src, dst, small_sem.at[3 + i]) for i, (src, dst) in enumerate((
        (source_h, source_v), (target_h, target_v), (count_h, count_s), (len_h, len_s), (em_h, em), (refl_h, refl)))]
    for copy in inputs[:4]:
        copy.start()
    for c in range(min(SLOTS, chunks)):
        fetch(c, c).start()
    for copy in inputs[4:]:
        copy.start()

    lane = lax.broadcasted_iota(i32, (1, 128), 1)

    for copy in inputs[:4]:
        copy.wait()
    owner, slot = divide(source_v[...], clusters)
    target = target_v[...] - me * clusters
    ids = lax.broadcasted_iota(i32, (1, blocks), 1)
    peers = lax.broadcasted_iota(i32, (n, blocks), 0)
    alive = jnp.broadcast_to(ids < count_s[0], (n, blocks))
    match = jnp.logical_and(owner == peers, alive)
    wanted = jnp.max(jnp.where(match, jnp.broadcast_to(slot, (n, blocks)), 0), axis=1, keepdims=True)
    wout[...] = jnp.broadcast_to(wanted, (n, 128)).reshape(n, 1, 128)
    pl.semaphore_wait(barrier, n - 1)

    each_peer(lambda px, py: pltpu.make_async_remote_copy(
        src_ref=wout.at[px * ny + py], dst_ref=win.at[me], send_sem=wsend_sem, recv_sem=wrecv_sem,
        device_id=(px, py), device_id_type=pl.DeviceIdType.MESH).start())
    win[me] = wout[me]

    square_of = (blocks, blocks)
    down = lax.broadcasted_iota(i32, square_of, 0)
    across = lax.broadcasted_iota(i32, square_of, 1)

    def upright(row):
        return jnp.sum(jnp.where(down == across, jnp.broadcast_to(row, square_of), 0), axis=1, keepdims=True)

    key = target * blocks + ids
    key_up, owner_up, target_up = upright(key), upright(owner), upright(target)
    rank = jnp.sum((jnp.broadcast_to(key, square_of) < key_up).astype(i32), axis=1, keepdims=True)
    placed = rank == across

    def ordered(column):
        return jnp.sum(jnp.where(placed, column, 0), axis=0, keepdims=True)

    sorted_target = ordered(jnp.broadcast_to(target_up, square_of))
    ints_v[...] = jnp.zeros(ints_v.shape, i32)
    reals_v[...] = jnp.zeros(reals_v.shape, f32)
    ints_v[0:1, :] = ordered(down)
    ints_v[1:2, :] = ordered(jnp.broadcast_to(owner_up, square_of))
    up_to = jnp.sum((target_up <= across).astype(i32), axis=0, keepdims=True)
    same = jnp.sum((target_up == across).astype(i32), axis=0, keepdims=True)
    ints_v[2:3, :] = jnp.maximum(up_to - 1, 0)
    shifted = pltpu.roll(jnp.broadcast_to(sorted_target, (8, blocks)), 1, 1)[0:1]
    joined = jnp.logical_and(shifted == sorted_target, ids > 0)
    reals_v[0:1, :] = jnp.where(joined, 1.0, 0.0)
    reals_v[1:2, :] = jnp.where(same > 0, 1.0, 0.0)
    small = (pltpu.make_async_copy(ints_v, ints_s, small_sem.at[0]),
             pltpu.make_async_copy(reals_v, reals_s, small_sem.at[1]))
    for copy in small:
        copy.start()

    def fold(pairs):
        parts = [jnp.sum(a * b, axis=0) for a, b in pairs]
        if len(parts) == 1:
            return jnp.sum(parts[0], axis=0, keepdims=True)
        row = jnp.zeros((1, 128), f32)
        for i, part in enumerate(parts):
            part = part + pltpu.roll(part, 64, 1)
            part = part + pltpu.roll(part, 32, 1)
            row = jnp.where(lane // 32 == i, jnp.sum(part, axis=0, keepdims=True), row)
        return row

    def send(phase, pick):
        def one(px, py):
            peer = px * ny + py
            outb[phase, peer] = pick(peer)
            pltpu.make_async_remote_copy(
                src_ref=outb.at[phase, peer], dst_ref=inb.at[phase, me],
                send_sem=send_sem.at[phase], recv_sem=recv_sem.at[phase],
                device_id=(px, py), device_id_type=pl.DeviceIdType.MESH).start()

        each_peer(one)
        inb[phase, me] = pick(me)

    def send_sums(phase, pairs):
        row = fold(pairs)
        dout[phase] = row
        each_peer(lambda px, py: pltpu.make_async_remote_copy(
            src_ref=dout.at[phase], dst_ref=din.at[phase, me],
            send_sem=ssend_sem.at[phase], recv_sem=srecv_sem.at[phase],
            device_id=(px, py), device_id_type=pl.DeviceIdType.MESH).start())
        din[phase, me] = row

    def drain(ref, sem):
        part = ref.at[pl.ds(0, n - 1)]
        pltpu.make_async_copy(part, part, sem).wait()

    def receive(phase):
        drain(inb.at[phase], recv_sem.at[phase])
        drain(outb.at[phase], send_sem.at[phase])

    def sums(phase, count):
        drain(din.at[phase], srecv_sem.at[phase])
        drain(din.at[phase], ssend_sem.at[phase])
        column = jnp.sum(din[phase], axis=0)
        out = []
        for i in range(count):
            part = column if count == 1 else jnp.where(lane // 32 == i, column, 0.0)
            out.append(jnp.broadcast_to(jnp.sum(part, axis=1, keepdims=True), (8, 128)))
        return out

    def put_sources(v):
        low = v - v.astype(bf16).astype(f32)
        vt[...] = jnp.concatenate([v, low], axis=1).astype(bf16)

    def apply(v):
        blank = jnp.zeros((16, cl), bf16)

        def step(s, acc):
            for u in range(UNROLL // 4):
                r = s * UNROLL + 4 * u
                va, vb, vc, vd = (vt[ints_s[1, r + j]] for j in range(4))
                wa, wb, wc, wd = (w[ints_s[0, r + j]] for j in range(4))
                left = jnp.concatenate([
                    jnp.concatenate([va, blank], axis=1), jnp.concatenate([blank, vb], axis=1),
                    jnp.concatenate([vc, blank], axis=1), jnp.concatenate([blank, vd], axis=1)], axis=0)
                right = jnp.concatenate([
                    jnp.concatenate([wa, wb], axis=0), jnp.concatenate([wc, wd], axis=0)], axis=1)
                out = jnp.dot(left, right, preferred_element_type=f32)
                for j in range(4):
                    half = out[:, 0:cl] if j < 2 else out[:, cl:2 * cl]
                    acc = acc * reals_s[0, r + j] + (half[16 * j:16 * j + 8] + half[16 * j + 8:16 * j + 16])
                    runs[r + j] = acc
            return acc

        lax.fori_loop(0, blocks // UNROLL, step, jnp.zeros((8, cl), f32))
        g = jnp.stack([runs[ints_s[2, t]] * reals_s[1, t] for t in range(clusters)])
        return v - refl[...] * g

    def prepare(c, carry):
        slot = lax.rem(c, SLOTS)
        fetch(c, slot).wait()

        def block(b, inner):
            k = c * CHUNK + b
            t = stage[slot, b].T
            limit = jnp.where(k < count_s[0], len_s[k], 0)
            j = lax.broadcasted_iota(jnp.int32, (16, cl), 0)
            error = jnp.zeros((16, cl), f32)
            for m in range(0, cl, 16):
                x = jnp.where(j < limit - m, t[m:m + 16] + error, 0.0)
                q = x.astype(bf16)
                w[k, m:m + 16] = q
                error = x - q.astype(f32)
            return inner

        lax.fori_loop(0, CHUNK, block, 0, unroll=4)

        @pl.when(c + SLOTS < chunks)
        def _():
            fetch(c + SLOTS, slot).start()

        return carry

    for copy in inputs[4:]:
        copy.wait()
    early = min(EARLY, chunks)
    lax.fori_loop(0, early, prepare, 0)
    drain(win, wrecv_sem)
    drain(wout, wsend_sem)
    asked = pltpu.make_async_copy(win, want_s, small_sem.at[2])
    asked.start()

    def chosen(peer):
        slots = jnp.broadcast_to(win[peer], (8, 128))
        v = em[0]
        for c in range(1, clusters):
            v = jnp.where(slots == c, em[c], v)
        return v

    send(0, chosen)
    send_sums(0, [(em[...], em[...])])
    lax.fori_loop(early, chunks, prepare, 0)
    for copy in small:
        copy.wait()
    asked.wait()

    receive(0)
    rs[...] = inb[0]
    res[...] = em[...]
    rho, rho_old, alpha, omega = None, None, None, None
    for it in range(ITERS):
        last = it == ITERS - 1
        if it == 0:
            direction[...] = em[...]
            ds[...] = rs[...]
        else:
            beta = rho / rho_old * (alpha / omega)
            direction[...] = res[...] + beta * (direction[...] - omega * image[...])
            ds[...] = rs[...] + beta * (ds[...] - omega * inb[2 * it - 1])
        put_sources(ds[...])
        image[...] = apply(direction[...])
        phase = 1 + 2 * it
        send(phase, lambda peer: image[want_s[peer, 0, 0]])
        send_sums(phase, [(em[...], image[...])])
        if it == 0:
            rho, = sums(0, 1)
        receive(phase)
        alpha = rho / sums(phase, 1)[0]
        rs[...] = rs[...] - alpha * inb[phase]
        put_sources(rs[...])
        res[...] = res[...] - alpha * image[...]
        sol[...] = apply(res[...])
        phase = phase + 1
        if not last:
            send(phase, lambda peer: sol[want_s[peer, 0, 0]])
        send_sums(phase, [(sol[...], res[...]), (sol[...], sol[...]), (em[...], res[...]), (em[...], sol[...])])
        if it == 0:
            total[...] = alpha * direction[...]
        else:
            total[...] = total[...] + alpha * direction[...]
        if not last:
            receive(phase)
        tm, tt, sm, st = sums(phase, 4)
        omega = tm / tt
        rho_old, rho = rho, sm - omega * st
        total[...] = total[...] + omega * res[...]
        res[...] = res[...] - omega * sol[...]
        if not last:
            rs[...] = rs[...] - omega * inb[phase]
    sol[...] = total[...]


def local(emission, reflectance, form_factors, link_source, link_target, link_length, block_count):
    clusters, bands, cl = emission.shape
    blocks = form_factors.shape[0]
    devices = lax.axis_size(("gx", "gy"))
    i32, f32, bf16 = jnp.int32, jnp.float32, jnp.bfloat16
    vmem = pl.BlockSpec(memory_space=pltpu.VMEM)
    field = (clusters, bands, cl)
    rows = (devices, bands, cl)
    dma = pltpu.SemaphoreType.DMA
    return pl.pallas_call(
        kernel,
        out_shape=[jax.ShapeDtypeStruct(field, f32)] * 2,
        in_specs=[pl.BlockSpec(memory_space=pl.ANY)] * 7,
        out_specs=[vmem, vmem],
        scratch_shapes=[
            pltpu.VMEM((blocks, cl, cl), bf16),
            pltpu.VMEM((SLOTS, CHUNK, cl, cl), f32),
            pltpu.VMEM((blocks, bands, cl), f32),
            pltpu.VMEM((devices, 2 * bands, cl), bf16),
            pltpu.VMEM((PHASES - 1, devices, bands, cl), f32),
            pltpu.VMEM((PHASES - 1, devices, bands, cl), f32),
            pltpu.VMEM((PHASES, 1, 128), f32),
            pltpu.VMEM((PHASES, devices, 1, 128), f32),
            pltpu.VMEM(field, f32),
            pltpu.VMEM(field, f32),
            pltpu.VMEM(field, f32),
            pltpu.VMEM(field, f32),
            pltpu.VMEM(field, f32),
            pltpu.VMEM(rows, f32),
            pltpu.VMEM(rows, f32),
            pltpu.VMEM((devices, 1, 128), i32),
            pltpu.VMEM((devices, 1, 128), i32),
            pltpu.SMEM((devices, 1, 128), i32),
            pltpu.VMEM((8, blocks), i32),
            pltpu.SMEM((8, blocks), i32),
            pltpu.VMEM((8, blocks), f32),
            pltpu.SMEM((8, blocks), f32),
            pltpu.VMEM((1, blocks), i32),
            pltpu.VMEM((1, blocks), i32),
            pltpu.SMEM((blocks,), i32),
            pltpu.SMEM((1,), i32),
            dma((SLOTS,)),
            dma((PHASES - 1,)),
            dma((PHASES - 1,)),
            dma((PHASES,)),
            dma((PHASES,)),
            dma,
            dma,
            dma((9,)),
        ],
        compiler_params=pltpu.CompilerParams(
            collective_id=0, has_side_effects=True, vmem_limit_bytes=VMEM_LIMIT),
        name="radiosity",
    )(link_length, block_count, link_source.reshape(1, blocks), link_target.reshape(1, blocks),
      emission, reflectance, form_factors)


VMEM_LIMIT = 56 * 1024 * 1024


def solution(mesh):
    wide = P(("gx", "gy"), None, None)
    flat = P(("gx", "gy"))
    return jax.shard_map(local, mesh=mesh, in_specs=(wide, wide, wide, flat, flat, flat, flat),
                         out_specs=(wide, wide), check_vma=False)
```

```python
import jax
import jax.numpy as jnp
from jax import lax
from jax.sharding import PartitionSpec as P
from jax.experimental import pallas as pl
from jax.experimental.pallas import tpu as pltpu

ITERS = 3
PHASES = 2 * ITERS + 1
CHUNK = 16
SLOTS = 4
UNROLL = 256
BEFORE = 2
EARLY = 9


def divide(x, by):
    if by & (by - 1) == 0:
        return lax.shift_right_logical(x, by.bit_length() - 1), lax.bitwise_and(x, by - 1)
    return lax.div(x, by), lax.rem(x, by)


def partners(index, size):
    if size & (size - 1):
        return [lax.rem(index + a, size) for a in range(size)]
    flips = [(1 << b) - 2 * (1 << b) * lax.rem(lax.div(index, 1 << b), 2) for b in range(size.bit_length() - 1)]
    out = []
    for a in range(size):
        p = index
        for b, flip in enumerate(flips):
            if a >> b & 1:
                p = p + flip
        out.append(p)
    return out


def kernel(count_s, len_h, source_h, target_h, em_h, refl_h, ff, total, res, sol, last_omega,
           w, stage, runs, vt, outb, inb, dout, din, em, refl, image, direction, rs, ds,
           wout, win, want_s, ints_v, ints_s, reals_v, reals_s, source_v, target_v, len_v, limit_v, limit_s,
           stage_sem, send_sem, recv_sem, ssend_sem, srecv_sem, wsend_sem, wrecv_sem, small_sem):
    nx, ny = lax.axis_size("gx"), lax.axis_size("gy")
    n = nx * ny
    gx, gy = lax.axis_index("gx"), lax.axis_index("gy")
    me = gx * ny + gy
    clusters = em.shape[0]
    blocks, cl = ff.shape[0], ff.shape[2]
    chunks = blocks // CHUNK
    i32, f32, bf16 = jnp.int32, jnp.float32, jnp.bfloat16

    pxs, pys = partners(gx, nx), partners(gy, ny)
    order = sorted(
        ((a, b) for a in range(nx) for b in range(ny) if a or b),
        key=lambda q: (-bin(q[0] >> 1).count("1") - (q[1] & 1), -(q[0] & 1), -q[1]))

    def each_peer(act):
        for a, b in order:
            act(pxs[a], pys[b])

    barrier = pltpu.get_barrier_semaphore()
    each_peer(lambda px, py: pl.semaphore_signal(
        barrier, inc=1, device_id=(px, py), device_id_type=pl.DeviceIdType.MESH))

    def fetch(c, slot):
        return pltpu.make_async_copy(ff.at[pl.ds(c * CHUNK, CHUNK)], stage.at[slot], stage_sem.at[slot])

    inputs = [pltpu.make_async_copy(src, dst, small_sem.at[3 + i]) for i, (src, dst) in enumerate((
        (source_h, source_v), (target_h, target_v), (len_h, len_v), (em_h, em), (refl_h, refl)))]
    for copy in inputs[:3]:
        copy.start()
    for c in range(min(SLOTS, chunks)):
        fetch(c, c).start()
    for copy in inputs[3:]:
        copy.start()

    lane = lax.broadcasted_iota(i32, (1, 128), 1)

    for copy in inputs[:3]:
        copy.wait()
    owner, slot = divide(source_v[...], clusters)
    target = target_v[...] - me * clusters
    ids = lax.broadcasted_iota(i32, (1, blocks), 1)
    peers = lax.broadcasted_iota(i32, (n, blocks), 0)
    live = ids < count_s[0]
    limit_v[...] = jnp.where(live, len_v[...], 0)
    limits = pltpu.make_async_copy(limit_v, limit_s, small_sem.at[9])
    limits.start()
    alive = jnp.broadcast_to(live, (n, blocks))
    match = jnp.logical_and(owner == peers, alive)
    wanted = jnp.max(jnp.where(match, jnp.broadcast_to(slot, (n, blocks)), 0), axis=1, keepdims=True)
    wout[...] = jnp.broadcast_to(wanted, (n, 128)).reshape(n, 1, 128)
    square_of = (blocks, blocks)
    down = lax.broadcasted_iota(i32, square_of, 0)
    across = lax.broadcasted_iota(i32, square_of, 1)

    def upright(row):
        return jnp.sum(jnp.where(down == across, jnp.broadcast_to(row, square_of), 0), axis=1, keepdims=True)

    key = target * blocks + ids
    key_up, owner_up, target_up = upright(key), upright(owner), upright(target)
    rank = jnp.sum((jnp.broadcast_to(key, square_of) < key_up).astype(i32), axis=1, keepdims=True)
    placed = rank == across

    def ordered(column):
        return jnp.sum(jnp.where(placed, column, 0), axis=0, keepdims=True)

    sorted_target = ordered(jnp.broadcast_to(target_up, square_of))
    ints_v[...] = jnp.zeros(ints_v.shape, i32)
    reals_v[...] = jnp.zeros(reals_v.shape, f32)
    ints_v[0:1, :] = ordered(down)
    ints_v[1:2, :] = ordered(jnp.broadcast_to(owner_up, square_of))
    up_to = jnp.sum((target_up <= across).astype(i32), axis=0, keepdims=True)
    same = jnp.sum((target_up == across).astype(i32), axis=0, keepdims=True)
    ints_v[2:3, :] = jnp.maximum(up_to - 1, 0)
    shifted = pltpu.roll(jnp.broadcast_to(sorted_target, (8, blocks)), 1, 1)[0:1]
    joined = jnp.logical_and(shifted == sorted_target, ids > 0)
    reals_v[0:1, :] = jnp.where(joined, 1.0, 0.0)
    reals_v[1:2, :] = jnp.where(same > 0, 1.0, 0.0)
    small = (pltpu.make_async_copy(ints_v, ints_s, small_sem.at[0]),
             pltpu.make_async_copy(reals_v, reals_s, small_sem.at[1]))
    for copy in small:
        copy.start()

    def prepare(c, carry):
        slot = lax.rem(c, SLOTS)
        fetch(c, slot).wait()

        def block(b, inner):
            k = c * CHUNK + b
            t = stage[slot, b].T
            limit = limit_s[0, k]
            j = lax.broadcasted_iota(jnp.int32, (16, cl), 0)
            error = jnp.zeros((16, cl), f32)
            for m in range(0, cl, 16):
                x = jnp.where(j < limit - m, t[m:m + 16] + error, 0.0)
                q = x.astype(bf16)
                w[k, m:m + 16] = q
                error = x - q.astype(f32)
            return inner

        lax.fori_loop(0, CHUNK, block, 0, unroll=4)

        @pl.when(c + SLOTS < chunks)
        def _():
            fetch(c + SLOTS, slot).start()

        return carry

    limits.wait()
    before = min(BEFORE, chunks)
    lax.fori_loop(0, before, prepare, 0)
    pl.semaphore_wait(barrier, n - 1)

    each_peer(lambda px, py: pltpu.make_async_remote_copy(
        src_ref=wout.at[px * ny + py], dst_ref=win.at[me], send_sem=wsend_sem, recv_sem=wrecv_sem,
        device_id=(px, py), device_id_type=pl.DeviceIdType.MESH).start())
    win[me] = wout[me]

    def fold(pairs):
        parts = [jnp.sum(a * b, axis=0) for a, b in pairs]
        if len(parts) == 1:
            return jnp.sum(parts[0], axis=0, keepdims=True)
        row = jnp.zeros((1, 128), f32)
        for i, part in enumerate(parts):
            part = part + pltpu.roll(part, 64, 1)
            part = part + pltpu.roll(part, 32, 1)
            row = jnp.where(lane // 32 == i, jnp.sum(part, axis=0, keepdims=True), row)
        return row

    def send(phase, pick):
        def one(px, py):
            peer = px * ny + py
            outb[phase, peer] = pick(peer)
            pltpu.make_async_remote_copy(
                src_ref=outb.at[phase, peer], dst_ref=inb.at[phase, me],
                send_sem=send_sem.at[phase], recv_sem=recv_sem.at[phase],
                device_id=(px, py), device_id_type=pl.DeviceIdType.MESH).start()

        each_peer(one)
        inb[phase, me] = pick(me)

    def send_sums(phase, pairs):
        row = fold(pairs)
        dout[phase] = row
        each_peer(lambda px, py: pltpu.make_async_remote_copy(
            src_ref=dout.at[phase], dst_ref=din.at[phase, me],
            send_sem=ssend_sem.at[phase], recv_sem=srecv_sem.at[phase],
            device_id=(px, py), device_id_type=pl.DeviceIdType.MESH).start())
        din[phase, me] = row

    def drain(ref, sem):
        part = ref.at[pl.ds(0, n - 1)]
        pltpu.make_async_copy(part, part, sem).wait()

    def receive(phase):
        drain(inb.at[phase], recv_sem.at[phase])
        drain(outb.at[phase], send_sem.at[phase])

    def sums(phase, count):
        drain(din.at[phase], srecv_sem.at[phase])
        drain(din.at[phase], ssend_sem.at[phase])
        parts = din[phase]
        column = jnp.sum(parts, axis=0)
        out = []
        for i in range(count):
            part = column if count == 1 else jnp.where(lane // 32 == i, column, 0.0)
            out.append(jnp.broadcast_to(jnp.sum(part, axis=1, keepdims=True), (8, 128)))
        return out if count == 1 else out + [parts.reshape(n, 128)]

    def put_sources(place, v):
        low = v - v.astype(bf16).astype(f32)
        vt[place] = jnp.concatenate([v, low], axis=1).astype(bf16)

    def gather(places):
        tall = 16 * len(places)
        blank = jnp.zeros((tall, cl), bf16)

        def step(s, accs):
            for u in range(UNROLL // 4):
                r = s * UNROLL + 4 * u
                owners = [ints_s[1, r + j] for j in range(4)]
                va, vb, vc, vd = (jnp.concatenate([vt[p, o] for p in places], axis=0) for o in owners)
                wa, wb, wc, wd = (w[ints_s[0, r + j]] for j in range(4))
                left = jnp.concatenate([
                    jnp.concatenate([va, blank], axis=1), jnp.concatenate([blank, vb], axis=1),
                    jnp.concatenate([vc, blank], axis=1), jnp.concatenate([blank, vd], axis=1)], axis=0)
                right = jnp.concatenate([
                    jnp.concatenate([wa, wb], axis=0), jnp.concatenate([wc, wd], axis=0)], axis=1)
                out = jnp.dot(left, right, preferred_element_type=f32)
                for j in range(4):
                    half = out[:, 0:cl] if j < 2 else out[:, cl:2 * cl]
                    new = []
                    for p, acc in zip(places, accs):
                        at = tall * j + 16 * len(new)
                        acc = acc * reals_s[0, r + j] + (half[at:at + 8] + half[at + 8:at + 16])
                        runs[p, r + j] = acc
                        new.append(acc)
                    accs = tuple(new)
            return accs

        lax.fori_loop(0, blocks // UNROLL, step, tuple(jnp.zeros((8, cl), f32) for _ in places))
        return [jnp.stack([runs[p, ints_s[2, t]] * reals_s[1, t] for t in range(clusters)]) for p in places]

    for copy in inputs[3:]:
        copy.wait()
    early = min(EARLY, chunks)
    lax.fori_loop(before, early, prepare, 0)
    drain(win, wrecv_sem)
    drain(wout, wsend_sem)
    asked = pltpu.make_async_copy(win, want_s, small_sem.at[2])
    asked.start()

    def chosen(peer):
        slots = jnp.broadcast_to(win[peer], (8, 128))
        v = em[0]
        for c in range(1, clusters):
            v = jnp.where(slots == c, em[c], v)
        return v

    send(0, chosen)
    send_sums(0, [(em[...], em[...])])
    lax.fori_loop(early, chunks, prepare, 0)
    for copy in small:
        copy.wait()
    asked.wait()

    receive(0)
    rs[...] = inb[0]
    res[...] = em[...]
    rho, rho_old, alpha, omega = None, None, None, None
    for it in range(ITERS):
        last = it == ITERS - 1
        if it == 0:
            direction[...] = em[...]
            ds[...] = rs[...]
        else:
            beta = rho / rho_old * (alpha / omega)
            direction[...] = res[...] + beta * (direction[...] - omega * image[...])
            ds[...] = rs[...] + beta * (ds[...] - omega * inb[2 * it - 1])
        put_sources(0, ds[...])
        image[...] = direction[...] - refl[...] * gather([0])[0]
        phase = 1 + 2 * it
        send(phase, lambda peer: image[want_s[peer, 0, 0]])
        send_sums(phase, [(em[...], image[...])])
        put_sources(0, rs[...])
        receive(phase)
        put_sources(1, inb[phase])
        g, h = gather([0, 1])
        if it == 0:
            rho, = sums(0, 1)
        alpha = rho / sums(phase, 1)[0]
        res[...] = res[...] - alpha * image[...]
        sol[...] = res[...] - refl[...] * (g - alpha * h)
        phase = phase + 1
        if not last:
            send(phase, lambda peer: sol[want_s[peer, 0, 0]])
        send_sums(phase, [(sol[...], res[...]), (sol[...], sol[...]), (em[...], res[...]), (em[...], sol[...])])
        rs[...] = rs[...] - alpha * inb[phase - 1]
        if it == 0:
            total[...] = alpha * direction[...]
        else:
            total[...] = total[...] + alpha * direction[...]
        if not last:
            receive(phase)
        tm, tt, parts = sums(phase, 2)
        omega = tm / tt
        if not last:
            parts = jnp.sum(parts - omega[0:1] * pltpu.roll(parts, 96, 1), axis=0, keepdims=True)
            parts = jnp.sum(jnp.where(lane // 32 == 2, parts, 0.0), axis=1, keepdims=True)
            rho_old, rho = rho, jnp.broadcast_to(parts, (8, 128))
        if last:
            last_omega[...] = omega
        else:
            total[...] = total[...] + omega * res[...]
            res[...] = res[...] - omega * sol[...]
            rs[...] = rs[...] - omega * inb[phase]


def local(emission, reflectance, form_factors, link_source, link_target, link_length, block_count):
    clusters, bands, cl = emission.shape
    blocks = form_factors.shape[0]
    devices = lax.axis_size(("gx", "gy"))
    i32, f32, bf16 = jnp.int32, jnp.float32, jnp.bfloat16
    vmem = pl.BlockSpec(memory_space=pltpu.VMEM)
    field = (clusters, bands, cl)
    rows = (devices, bands, cl)
    dma = pltpu.SemaphoreType.DMA
    total, middle, bounce, omega = pl.pallas_call(
        kernel,
        out_shape=[jax.ShapeDtypeStruct(field, f32)] * 3 + [jax.ShapeDtypeStruct((bands, cl), f32)],
        in_specs=[pl.BlockSpec(memory_space=pltpu.SMEM)] + [pl.BlockSpec(memory_space=pl.ANY)] * 6,
        out_specs=[vmem] * 4,
        scratch_shapes=[
            pltpu.VMEM((blocks, cl, cl), bf16),
            pltpu.VMEM((SLOTS, CHUNK, cl, cl), f32),
            pltpu.VMEM((2, blocks, bands, cl), f32),
            pltpu.VMEM((2, devices, 2 * bands, cl), bf16),
            pltpu.VMEM((PHASES - 1, devices, bands, cl), f32),
            pltpu.VMEM((PHASES - 1, devices, bands, cl), f32),
            pltpu.VMEM((PHASES, 1, 128), f32),
            pltpu.VMEM((PHASES, devices, 1, 128), f32),
            pltpu.VMEM(field, f32),
            pltpu.VMEM(field, f32),
            pltpu.VMEM(field, f32),
            pltpu.VMEM(field, f32),
            pltpu.VMEM(rows, f32),
            pltpu.VMEM(rows, f32),
            pltpu.VMEM((devices, 1, 128), i32),
            pltpu.VMEM((devices, 1, 128), i32),
            pltpu.SMEM((devices, 1, 128), i32),
            pltpu.VMEM((8, blocks), i32),
            pltpu.SMEM((8, blocks), i32),
            pltpu.VMEM((8, blocks), f32),
            pltpu.SMEM((8, blocks), f32),
            pltpu.VMEM((1, blocks), i32),
            pltpu.VMEM((1, blocks), i32),
            pltpu.VMEM((1, blocks), i32),
            pltpu.VMEM((1, blocks), i32),
            pltpu.SMEM((1, blocks), i32),
            dma((SLOTS,)),
            dma((PHASES - 1,)),
            dma((PHASES - 1,)),
            dma((PHASES,)),
            dma((PHASES,)),
            dma,
            dma,
            dma((10,)),
        ],
        compiler_params=pltpu.CompilerParams(
            collective_id=0, has_side_effects=True, vmem_limit_bytes=VMEM_LIMIT),
        name="radiosity",
    )(block_count, *(pltpu.with_memory_space_constraint(x, pltpu.HBM) for x in (
        link_length.reshape(1, blocks), link_source.reshape(1, blocks), link_target.reshape(1, blocks),
        emission, reflectance, form_factors)))
    return total + omega * middle, middle - omega * bounce


VMEM_LIMIT = 24 * 1024 * 1024


def solution(mesh):
    wide = P(("gx", "gy"), None, None)
    flat = P(("gx", "gy"))
    return jax.shard_map(local, mesh=mesh, in_specs=(wide, wide, wide, flat, flat, flat, flat),
                         out_specs=(wide, wide), check_vma=False)
```
